32 devices in a mesh: slab: 4 (over y, core), pencil: 8 (over z, x).
Axes of the slice: x: 2, y: 2, z: 4, core: 2. Of those that a mesh axis runs over, the one named last changes fastest.
Arguments:
- density: float32 [128, 768, 512], P('pencil', None, 'slab'), may hold values from -6 to 6
- source: float32 [128, 768, 512], P('pencil', None, 'slab'), may hold values from -6 to 8
- coupling: float32 [3], replicated, may hold values from 0.25 to 2, as said below
- width_inverse: float32 [6, 128, 128], replicated, as said below
- height_inverse: float32 [1, 128, 128], replicated, as said below
- depth_inverse: float32 [4, 128, 128], replicated, as said below
Outputs:
- stepped: float32 [128, 768, 512], P('pencil', None, 'slab')
The draws below stay inside these ranges and needn't reach their ends.
Inputs may be any that keep to these rules, and one draw needn't show every extreme that they name: coupling holds three positive coefficients. `width_inverse`: block i is the inverse of the i-th pivot block of the block LU factorization of the tridiagonal line matrix with diagonal 1 + 2 s and off-diagonals -s, s the matching coupling. `height_inverse`: as for width_inverse, for the height lines. `depth_inverse`: as for width_inverse, for the depth lines.
All inputs are finite; a program needn't handle non-finite values.
Results may differ from the reference program's by a relative error of at most 0.00027.
Values sent between devices are 32-bit elements; how exact they have to be, the bound alone decides.
A program may use at most 128 MiB of HBM per device.

```python
import jax
import jax.numpy as jnp
from jax import lax

BLOCK = 128
NX = 768
NY = 128
NZ = 512


def coupling_values(key):
    folded = jax.random.fold_in(key, 7)
    uniform_draw = jax.random.uniform(folded, (3,), jnp.float32)
    return 0.25 * jnp.exp(uniform_draw * jnp.log(8.0))


def block_inverses(strength, count):
    identity = jnp.eye(BLOCK, dtype=jnp.float32)
    beside = jnp.eye(BLOCK, k=1, dtype=jnp.float32) + jnp.eye(BLOCK, k=-1, dtype=jnp.float32)
    tridiag = (1.0 + 2.0 * strength) * identity - strength * beside
    corner_unit = jnp.zeros((BLOCK, BLOCK), jnp.float32).at[0, 0].set(1.0)
    matrices = []
    corner = jnp.float32(0.0)
    for number in range(count):
        pivot = tridiag - strength * strength * corner * corner_unit
        inverse = jnp.linalg.inv(pivot)
        matrices.append(inverse)
        corner = inverse[BLOCK - 1, BLOCK - 1]
    return jnp.stack(matrices)


def draw_source(key, part):
    rough = jnp.clip(jax.random.normal(jax.random.fold_in(key, 11), (NY, NX, NZ), jnp.float32), -6.0, 6.0)
    return rough


def draw_coupling(key, part):
    return coupling_values(key)


def draw_width_inverse(key, part):
    return block_inverses(coupling_values(key)[0], NX // BLOCK)


def draw_height_inverse(key, part):
    return block_inverses(coupling_values(key)[1], NY // BLOCK)


def draw_depth_inverse(key, part):
    return block_inverses(coupling_values(key)[2], NZ // BLOCK)


def levels(own_key, dims, split, low, largest):
    def one(position, parts):
        heights = jax.random.uniform(jax.random.fold_in(jax.random.fold_in(own_key, 6), position), (parts,), jnp.float32, low / len(split), largest / len(split))
        return jnp.repeat(jnp.exp(heights), dims[position] // parts).reshape((-1,) + (1,) * (len(dims) - position - 1))

    gain = one(*split[0])
    for cut in split[1:]:
        gain = gain * one(*cut)
    return gain


def bell_draw(own_key, extent, deviation, most, pieces=(), kind=jnp.bfloat16):
    values = jax.random.normal(own_key, extent, jnp.float32) * deviation
    if len(pieces) > 0:
        values = levels(own_key, extent, pieces, -0.22, 0.18) * values
    return jnp.clip(values, min=-most, max=most).astype(kind)


def setup_inputs(seed: int = 0) -> dict:
    streams_of = jax.random.split(jax.random.key(seed), 7)
    return {
        "density": bell_draw(streams_of[0], (NY, NX, NZ), 1.0, 6.0, ((0, 8), (2, 4)), jnp.float32),
        "source": draw_source(jax.random.fold_in(streams_of[6], 71), 0),
        "coupling": draw_coupling(jax.random.fold_in(streams_of[6], 71), 0),
        "width_inverse": draw_width_inverse(jax.random.fold_in(streams_of[6], 71), 0),
        "height_inverse": draw_height_inverse(jax.random.fold_in(streams_of[6], 71), 0),
        "depth_inverse": draw_depth_inverse(jax.random.fold_in(streams_of[6], 71), 0),
    }


def solve_inner(rhs, inverses, strength):
    outer, length, inner = rhs.shape
    size = inverses.shape[1]
    count = length // size
    blocked = rhs.reshape(outer, count, size, inner)

    def forward(current, state):
        result, carry = state
        piece = lax.dynamic_index_in_dim(blocked, current, 1, keepdims=False)
        matrix = lax.dynamic_index_in_dim(inverses, current, 0, keepdims=False)
        value = jnp.einsum('pkq,jk->pjq', piece, matrix, precision=lax.Precision.HIGHEST)
        value = value + strength * matrix[:, 0][None, :, None] * carry[:, None, :]
        result = lax.dynamic_update_index_in_dim(result, value, current, 1)
        return (result, value[:, size - 1, :])
    start = (jnp.zeros_like(blocked), jnp.zeros((outer, inner), blocked.dtype))
    halfway, unused = lax.fori_loop(0, count, forward, start)

    def backward(step, state):
        result, carry = state
        current = count - 1 - step
        value = lax.dynamic_index_in_dim(result, current, 1, keepdims=False)
        matrix = lax.dynamic_index_in_dim(inverses, current, 0, keepdims=False)
        value = value + strength * matrix[:, size - 1][None, :, None] * carry[:, None, :]
        result = lax.dynamic_update_index_in_dim(result, value, current, 1)
        return (result, value[:, 0, :])
    final, unused = lax.fori_loop(0, count, backward, (halfway, jnp.zeros((outer, inner), blocked.dtype)))
    return final.reshape(outer, length, inner)

def solve_last(rhs, inverses, strength):
    rows, length = rhs.shape
    size = inverses.shape[1]
    count = length // size
    blocked = rhs.reshape(rows, count, size)

    def forward(current, state):
        result, carry = state
        piece = lax.dynamic_index_in_dim(blocked, current, 1, keepdims=False)
        matrix = lax.dynamic_index_in_dim(inverses, current, 0, keepdims=False)
        value = jnp.einsum('pk,jk->pj', piece, matrix, precision=lax.Precision.HIGHEST)
        value = value + strength * matrix[:, 0][None, :] * carry[:, None]
        result = lax.dynamic_update_index_in_dim(result, value, current, 1)
        return (result, value[:, size - 1])
    halfway, unused = lax.fori_loop(0, count, forward, (jnp.zeros_like(blocked), jnp.zeros((rows,), blocked.dtype)))

    def backward(step, state):
        result, carry = state
        current = count - 1 - step
        value = lax.dynamic_index_in_dim(result, current, 1, keepdims=False)
        matrix = lax.dynamic_index_in_dim(inverses, current, 0, keepdims=False)
        value = value + strength * matrix[:, size - 1][None, :] * carry[:, None]
        result = lax.dynamic_update_index_in_dim(result, value, current, 1)
        return (result, value[:, 0])
    final, unused = lax.fori_loop(0, count, backward, (halfway, jnp.zeros((rows,), blocked.dtype)))
    return final.reshape(rows, length)

def second_difference(values, axis):
    widths = [(0, 0), (0, 0), (0, 0)]
    widths[axis] = (1, 1)
    padded = jnp.pad(values, widths)
    length = values.shape[axis]
    upper = lax.slice_in_dim(padded, 2, length + 2, axis=axis)
    lower = lax.slice_in_dim(padded, 0, length, axis=axis)
    return upper + lower - 2.0 * values

def reference(density, source, coupling, width_inverse, height_inverse, depth_inverse):
    along_width = second_difference(density, 1)
    along_height = second_difference(density, 0)
    along_depth = second_difference(density, 2)
    explicit = 2.0 * (coupling[0] * along_width + coupling[1] * along_height + coupling[2] * along_depth) + source
    width_step = solve_inner(explicit, width_inverse, coupling[0])
    height_step = solve_inner(width_step.reshape(1, NY, NX * NZ), height_inverse, coupling[1]).reshape(NY, NX, NZ)
    depth_step = solve_last(height_step.reshape(NY * NX, NZ), depth_inverse, coupling[2]).reshape(NY, NX, NZ)
    return density + depth_step
```

```python
import jax
import jax.numpy as jnp
from jax import lax
from jax.experimental import pallas as pl
from jax.experimental.pallas import tpu as pltpu
from jax.sharding import PartitionSpec as P

F32, BF16 = jnp.float32, jnp.bfloat16


def split(value):
    high = value.astype(BF16)
    return high, (value - high.astype(F32)).astype(BF16)


def split_outside(value):
    high = lax.reduce_precision(value, 8, 7)
    return high.astype(BF16), (value - high).astype(BF16)


def both(value, axis):
    return jnp.concatenate(split(value), axis=axis)


def dot(a, b, dims):
    return lax.dot_general(a, b, (dims, ((), ())), preferred_element_type=F32)


def ends_of(plane):
    depth = plane.shape[1]
    row = lax.broadcasted_iota(jnp.int32, (16, 2 * depth), 0)
    lane = lax.broadcasted_iota(jnp.int32, (16, 2 * depth), 1) % depth
    pick = ((row == 0) & (lane == 0)) | ((row == 1) & (lane == depth - 1))
    chosen = dot(pick.astype(F32).astype(BF16), both(plane, 1), ((1,), (1,)))
    return chosen[:2]


def rows_of(pieces, width):
    row = lax.broadcasted_iota(jnp.int32, (16, width), 0)
    value = jnp.zeros((16, width), F32)
    for number, piece in enumerate(pieces):
        value = jnp.where(row == number, piece.astype(F32), value)
    return value.astype(BF16)


def ends_kernel(rho_ref, ends_ref):
    ends_ref[0] = ends_of(rho_ref[0])


def height_kernel(planes, coupling, pivots, rho_ref, source_ref, halo_ref, x_ref, faces_ref):
    j = pl.program_id(0)
    rho = rho_ref[0]
    width, depth = rho.shape
    row = lax.broadcasted_iota(jnp.int32, rho.shape, 0)
    lane = lax.broadcasted_iota(jnp.int32, rho.shape, 1)
    below = jnp.where(row == 0, 0.0, pltpu.roll(rho, 1, 0))
    above = jnp.where(row == width - 1, 0.0, pltpu.roll(rho, width - 1, 0))
    before = jnp.where(lane == 0, 0.0, pltpu.roll(rho, 1, 1))
    after = jnp.where(lane == depth - 1, 0.0, pltpu.roll(rho, depth - 1, 1))
    left_high, left_low = split(halo_ref[0, 0:1])
    right_high, right_low = split(halo_ref[0, 1:2])
    first = (lax.broadcasted_iota(jnp.int32, (1, depth), 1) == 0).astype(F32)
    last = (lax.broadcasted_iota(jnp.int32, (1, depth), 1) == depth - 1).astype(F32)
    edge = dot(
        rows_of((left_high, left_low, right_high, right_low), width),
        rows_of((first, first, last, last), depth),
        ((0,), (0,)),
    )
    rhs = (
        2.0
        * (
            coupling[0] * (below + above - 2.0 * rho)
            + coupling[2] * (before + after + edge - 2.0 * rho)
        )
        + source_ref[0]
        + 2.0 * rho
    )
    strength = coupling[1]

    @pl.when(j == 0)
    def _():
        x_ref[0] = rhs * pivots[0]

    @pl.when(j > 0)
    def _():
        x_ref[j] = (rhs + strength * x_ref[jnp.maximum(j - 1, 0)]) * pivots[j]

    @pl.when(j == planes - 1)
    def _():
        shape = faces_ref.shape
        faces_ref[:, 0] = x_ref[planes - 1].reshape(shape[0], shape[2], shape[3])

        def back(step, unused):
            i = planes - 2 - step
            x_ref[i] = x_ref[i] + (strength * pivots[i]) * x_ref[i + 1]
            return unused

        lax.fori_loop(0, planes - 1, back, 0)
        faces_ref[:, 1] = x_ref[0].reshape(shape[0], shape[2], shape[3])


def lines_kernel(
    group, coupling, into, x_ref, rho_ref, faces_ref, width_ref, mixed_ref, depth_ref, z_ref, ends_ref
):
    j = pl.program_id(0)
    width, depth = x_ref.shape[1:]
    count, size = width_ref.shape[:2]
    enter = faces_ref[:, 0].reshape(width, depth)
    leave = faces_ref[:, 1].reshape(width, depth)
    rhs = jnp.concatenate(
        [
            x_ref[g]
            + into[0, j * group + g] * enter
            + into[1, j * group + g] * leave
            - 2.0 * rho_ref[g]
            for g in range(group)
        ],
        axis=1,
    )
    high, low = split(rhs)
    local, starts, stops = [], [], []
    for i in range(count):
        part = slice(i * size, (i + 1) * size)
        product = dot(mixed_ref[i], jnp.concatenate([high[part], low[part]], 0), ((1,), (0,)))
        local.append(product[:size] + product[size:])
        starts.append(coupling[0] * width_ref[i, :, 0:1])
        stops.append(coupling[0] * width_ref[i, :, size - 1 : size])
    carry = jnp.zeros((1, group * depth), F32)
    ahead, heads = [], []
    for i in range(count):
        ahead.append(carry)
        heads.append(local[i][0:1] + starts[i][0:1] * carry)
        carry = local[i][size - 1 :] + starts[i][size - 1 :] * carry
    carry = jnp.zeros((1, group * depth), F32)
    solved = [None] * count
    for i in reversed(range(count)):
        solved[i] = local[i] + starts[i] * ahead[i] + stops[i] * carry
        carry = heads[i] + stops[i][0:1] * carry
    solved = jnp.concatenate(solved, axis=0)
    for g in range(group):
        product = dot(both(solved[:, g * depth : (g + 1) * depth], 1), depth_ref[...], ((1,), (0,)))
        z = product[:, :depth] + product[:, depth:]
        z_ref[g] = z
        ends_ref[g] = ends_of(z)


def finish_kernel(group, rho_ref, z_ref, carry_ref, edge_ref, out_ref):
    width, depth = rho_ref.shape[1:]
    in_high, in_low = split(edge_ref[0:1])
    next_high, next_low = split(edge_ref[1:2])
    rhs = rows_of((in_high, in_high, in_low, next_high, next_high, next_low), depth)
    for g in range(group):
        a_high, a_low = split(carry_ref[g, 0:1])
        b_high, b_low = split(carry_ref[g, 1:2])
        lhs = rows_of((a_high, a_low, a_high, b_high, b_low, b_high), width)
        out_ref[g] = rho_ref[g] + z_ref[g] + dot(lhs, rhs, ((0,), (0,)))


def height_tables(strength, planes, count):
    root = (1.0 + 2.0 * strength + jnp.sqrt(1.0 + 4.0 * strength)) * 0.5
    ratio = strength / root
    log_ratio = jnp.log(ratio)

    def tail(index):
        return 1.0 - jnp.exp((2.0 * (index + 1.0)) * log_ratio)

    def power(index):
        return jnp.exp(index * log_ratio)

    base = (jnp.arange(count, dtype=F32) * planes)[:, None]
    j = jnp.arange(planes, dtype=F32)[None, :]
    pivots = tail(base + j) / (root * tail(base + j + 1.0))
    leave = power(planes - j) * tail(base + j) / tail(base + planes)
    base3, j3, m3 = base[:, :, None], j[:, :, None], j[:, None, :]
    distance = jnp.maximum(m3 - j3, 0.0)
    terms = (
        power(distance + m3 + 1.0)
        * (tail(base3 + j3) / tail(base3 + m3))
        * (tail(base3) / tail(base3 + m3 + 1.0))
    )
    enter = jnp.sum(jnp.where(m3 >= j3, terms, 0.0), axis=2)
    through = power(float(planes)) * tail(base[:, 0]) / tail(base[:, 0] + planes)
    return pivots, enter, leave, through


def per_device(density, source, coupling, width_inverse, height_inverse, depth_inverse):
    planes, width, depth = density.shape
    pencils, slabs = lax.axis_size("pencil"), lax.axis_size("slab")
    pencil, slab = lax.axis_index("pencil"), lax.axis_index("slab")
    size = depth_inverse.shape[1]
    group = 2
    smem = pl.BlockSpec(memory_space=pltpu.SMEM)
    params = pltpu.CompilerParams(
        dimension_semantics=("arbitrary",), vmem_limit_bytes=56 * 1024 * 1024
    )

    def whole(shape):
        return pl.BlockSpec(shape, lambda j: (0,) * len(shape))

    def per_plane(shape):
        return pl.BlockSpec(shape, lambda j: (j,) + (0,) * (len(shape) - 1))

    ends = pl.pallas_call(
        ends_kernel,
        grid=(planes,),
        out_shape=jax.ShapeDtypeStruct((planes, 2, width), F32),
        in_specs=[per_plane((1, width, depth))],
        out_specs=per_plane((1, 2, width)),
        compiler_params=params,
    )(density)
    up = [(i, i + 1) for i in range(slabs - 1)]
    down = [(i + 1, i) for i in range(slabs - 1)]
    left = lax.ppermute(ends[:, 1:2], "slab", up)
    right = lax.ppermute(ends[:, 0:1], "slab", down)
    halo = jnp.concatenate([left, right], axis=1)

    pivots, enter, leave, through = height_tables(coupling[1], planes, pencils)
    own_pivots = lax.dynamic_index_in_dim(pivots, pencil, 0, False)
    into = jnp.stack(
        [
            lax.dynamic_index_in_dim(enter, pencil, 0, False),
            lax.dynamic_index_in_dim(leave, pencil, 0, False),
        ]
    )
    share = width // pencils
    partial, faces = pl.pallas_call(
        lambda *refs: height_kernel(planes, *refs),
        grid=(planes,),
        out_shape=(
            jax.ShapeDtypeStruct((planes, width, depth), F32),
            jax.ShapeDtypeStruct((pencils, 2, share, depth), F32),
        ),
        in_specs=[
            smem,
            smem,
            per_plane((1, width, depth)),
            per_plane((1, width, depth)),
            per_plane((1, 2, width)),
        ],
        out_specs=(whole((planes, width, depth)), whole((pencils, 2, share, depth))),
        compiler_params=params,
    )(coupling, own_pivots, density, source, halo)

    held = lax.all_to_all(faces, "pencil", split_axis=0, concat_axis=0, tiled=True)
    entering = [jnp.zeros_like(held[0, 0])]
    for d in range(pencils - 1):
        entering.append(held[d, 0] + through[d] * entering[d])
    following = [None] * pencils
    following[pencils - 1] = jnp.zeros_like(held[0, 0])
    for d in range(pencils - 1, 0, -1):
        following[d - 1] = held[d, 1] + enter[d, 0] * entering[d] + leave[d, 0] * following[d]
    solved = jnp.stack([jnp.stack(pair) for pair in zip(entering, following)])
    solved = lax.all_to_all(solved, "pencil", split_axis=0, concat_axis=0, tiled=True)

    w_high, w_low = split_outside(width_inverse)
    mixed = jnp.concatenate(
        [
            jnp.concatenate([w_high, w_high], axis=2),
            jnp.concatenate([w_low, jnp.zeros_like(w_low)], axis=2),
        ],
        axis=1,
    )
    matrix = lax.dynamic_index_in_dim(depth_inverse, slab, 0, False).T
    d_high, d_low = split_outside(matrix)
    depth_mixed = jnp.concatenate(
        [
            jnp.concatenate([d_high, d_low], axis=1),
            jnp.concatenate([d_high, jnp.zeros_like(d_low)], axis=1),
        ],
        axis=0,
    )
    local, bounds = pl.pallas_call(
        lambda *refs: lines_kernel(group, *refs),
        grid=(planes // group,),
        out_shape=(
            jax.ShapeDtypeStruct((planes, width, depth), F32),
            jax.ShapeDtypeStruct((planes, 2, width), F32),
        ),
        in_specs=[
            smem,
            smem,
            per_plane((group, width, depth)),
            per_plane((group, width, depth)),
            whole(solved.shape),
            whole(width_inverse.shape),
            whole(mixed.shape),
            whole(depth_mixed.shape),
        ],
        out_specs=(per_plane((group, width, depth)), per_plane((group, 2, width))),
        compiler_params=params,
    )(coupling, into, partial, density, solved, width_inverse, mixed, depth_mixed)

    gathered = lax.all_gather(bounds, "slab")
    strength = coupling[2]
    zero = jnp.zeros((planes, width), F32)
    forward = [zero]
    for d in range(slabs - 1):
        forward.append(gathered[d, :, 1] + strength * depth_inverse[d, size - 1, 0] * forward[d])
    backward = [zero] * slabs
    for d in range(slabs - 1, 0, -1):
        backward[d - 1] = (
            gathered[d, :, 0]
            + strength * depth_inverse[d, 0, 0] * forward[d]
            + strength * depth_inverse[d, 0, size - 1] * backward[d]
        )
    carry_in, carry_next = forward[0], backward[0]
    for d in range(1, slabs):
        carry_in = jnp.where(slab == d, forward[d], carry_in)
        carry_next = jnp.where(slab == d, backward[d], carry_next)
    carries = jnp.stack([carry_in, carry_next], axis=1)
    edges = strength * jnp.stack([matrix[0], matrix[size - 1]])
    return pl.pallas_call(
        lambda *refs: finish_kernel(group, *refs),
        grid=(planes // group,),
        out_shape=jax.ShapeDtypeStruct((planes, width, depth), F32),
        in_specs=[
            per_plane((group, width, depth)),
            per_plane((group, width, depth)),
            per_plane((group, 2, width)),
            whole((2, depth)),
        ],
        out_specs=per_plane((group, width, depth)),
        compiler_params=params,
    )(density, local, carries, edges)


def solution(mesh):
    in_specs = (P("pencil", None, "slab"), P("pencil", None, "slab"), P(), P(), P(), P())
    out_specs = P("pencil", None, "slab")
    return jax.shard_map(
        per_device, mesh=mesh, in_specs=in_specs, out_specs=out_specs, check_vma=False
    )
```

```python
import jax
import jax.numpy as jnp
from jax import lax
from jax.experimental import pallas as pl
from jax.experimental.pallas import tpu as pltpu
from jax.sharding import PartitionSpec as P

F32, BF16 = jnp.float32, jnp.bfloat16
MESH = pl.DeviceIdType.MESH


def split(value):
    high = value.astype(BF16)
    return high, (value - high.astype(F32)).astype(BF16)


def split_outside(value):
    high = lax.reduce_precision(value, 8, 7)
    return high.astype(BF16), (value - high).astype(BF16)


def both(value, axis):
    return jnp.concatenate(split(value), axis=axis)


def dot(a, b, dims):
    return lax.dot_general(a, b, (dims, ((), ())), preferred_element_type=F32)


def ends_of(plane):
    width, depth = plane.shape
    row = lax.broadcasted_iota(jnp.int32, (depth, depth), 0)
    lane = lax.broadcasted_iota(jnp.int32, (depth, depth), 1)
    lines = []
    for column in (0, depth - 1):
        pieces = []
        for start in range(0, width, depth):
            edge = plane[start : start + depth, column : column + 1]
            pieces.append(jnp.sum(jnp.where(row == lane, edge, 0.0), axis=0, keepdims=True))
        lines.append(jnp.concatenate(pieces, axis=1))
    return jnp.concatenate(lines, axis=0)


def rows_of(pieces, width):
    row = lax.broadcasted_iota(jnp.int32, (16, width), 0)
    value = jnp.zeros((16, width), F32)
    for number, piece in enumerate(pieces):
        value = jnp.where(row == number, piece.astype(F32), value)
    return value.astype(BF16)


def ends_kernel(slabs, group, rho_ref, halo_ref, ends_ref, got_ref, send_sem, recv_sem):
    j = pl.program_id(0)
    me = lax.axis_index("slab")
    nxt, prv = lax.rem(me + 1, slabs), lax.rem(me + slabs - 1, slabs)
    barrier = pltpu.get_barrier_semaphore()

    @pl.when(j == 0)
    def _():
        for peer in (nxt, prv):
            pl.semaphore_signal(barrier, inc=1, device_id={"slab": peer}, device_id_type=MESH)
        pl.semaphore_wait(barrier, 2)

    for g in range(group):
        pair = ends_of(rho_ref[g])
        ends_ref[0, j * group + g] = pair[0:1]
        ends_ref[1, j * group + g] = pair[1:2]

    @pl.when(j == pl.num_programs(0) - 1)
    def _():
        copies = [
            pltpu.make_async_remote_copy(
                src_ref=ends_ref.at[1 - way],
                dst_ref=got_ref.at[way],
                send_sem=send_sem.at[way],
                recv_sem=recv_sem.at[way],
                device_id={"slab": peer},
                device_id_type=MESH,
            )
            for way, peer in ((0, nxt), (1, prv))
        ]
        for copy in copies:
            copy.start()
        for copy in copies:
            copy.wait()
        halo_ref[0] = jnp.where(me == 0, 0.0, got_ref[0])
        halo_ref[1] = jnp.where(me == slabs - 1, 0.0, got_ref[1])


def height_kernel(
    planes, group, coupling, pivots, rho_ref, source_ref, halo_ref, x_ref, faces_ref, kept_ref
):
    step = pl.program_id(0)
    width, depth = rho_ref.shape[1:]
    strength = coupling[1]
    row = lax.broadcasted_iota(jnp.int32, (width, depth), 0)
    lane = lax.broadcasted_iota(jnp.int32, (width, depth), 1)
    first = (lax.broadcasted_iota(jnp.int32, (1, depth), 1) == 0).astype(F32)
    last = (lax.broadcasted_iota(jnp.int32, (1, depth), 1) == depth - 1).astype(F32)
    units = rows_of((first, first, last, last), depth)

    @pl.when(step == 0)
    def _():
        x_ref[planes - 1] = jnp.zeros((width, depth), F32)

    for g in range(group):
        j = step * group + g
        rho = rho_ref[g]
        below = jnp.where(row == 0, 0.0, pltpu.roll(rho, 1, 0))
        above = jnp.where(row == width - 1, 0.0, pltpu.roll(rho, width - 1, 0))
        before = jnp.where(lane == 0, 0.0, pltpu.roll(rho, 1, 1))
        after = jnp.where(lane == depth - 1, 0.0, pltpu.roll(rho, depth - 1, 1))
        left_high, left_low = split(halo_ref[0, g])
        right_high, right_low = split(halo_ref[1, g])
        edge = dot(rows_of((left_high, left_low, right_high, right_low), width), units, ((0,), (0,)))
        rhs = (
            2.0
            * (
                coupling[0] * (below + above - 2.0 * rho)
                + coupling[2] * (before + after + edge - 2.0 * rho)
            )
            + source_ref[g]
            + 2.0 * rho
        )
        kept_ref[j] = 2.0 * rho
        x_ref[j] = (rhs + strength * x_ref[lax.rem(j + planes - 1, planes)]) * pivots[j]

    @pl.when(step == planes // group - 1)
    def _():
        shape = faces_ref.shape
        faces_ref[:, 0] = x_ref[planes - 1].reshape(shape[0], shape[2], shape[3])

        def back(count, unused):
            i = planes - 2 - count
            later = x_ref[i + 1]
            x_ref[i] = x_ref[i] + (strength * pivots[i]) * later
            x_ref[i + 1] = later - kept_ref[i + 1]
            return unused

        lax.fori_loop(0, planes - 1, back, 0)
        faces_ref[:, 1] = x_ref[0].reshape(shape[0], shape[2], shape[3])
        x_ref[0] = x_ref[0] - kept_ref[0]


def solve_group(rhs, strength, width_ref, mixed_ref, depth_mixed):
    count, size = width_ref.shape[:2]
    depth = size
    total = rhs.shape[1]
    high, low = split(rhs)
    local, starts, stops = [], [], []
    for i in range(count):
        part = slice(i * size, (i + 1) * size)
        product = dot(mixed_ref[i], jnp.concatenate([high[part], low[part]], 0), ((1,), (0,)))
        local.append(product[:size] + product[size:])
        starts.append(strength * width_ref[i, :, 0:1])
        stops.append(strength * width_ref[i, :, size - 1 : size])
    carry = jnp.zeros((1, total), F32)
    ahead, heads = [], []
    for i in range(count):
        ahead.append(carry)
        heads.append(local[i][0:1] + starts[i][0:1] * carry)
        carry = local[i][size - 1 :] + starts[i][size - 1 :] * carry
    carry = jnp.zeros((1, total), F32)
    solved = [None] * count
    for i in reversed(range(count)):
        solved[i] = local[i] + starts[i] * ahead[i] + stops[i] * carry
        carry = heads[i] + stops[i][0:1] * carry
    solved = jnp.concatenate(solved, axis=0)
    answers = []
    for start in range(0, total, depth):
        product = dot(both(solved[:, start : start + depth], 1), depth_mixed, ((1,), (0,)))
        answers.append(product[:, :depth] + product[:, depth:])
    return answers


def lines_kernel(
    group, pencils, slabs,
    coupling, into, chain, links,
    u_ref, faces_ref, width_ref, mixed_ref, depth_ref,
    z_ref, carry_ref,
    held, solved, final, face_z, ends, gathered,
    send_one, recv_one, send_two, recv_two, send_three, recv_three,
):
    planes, width, depth = u_ref.shape
    me, slab = lax.axis_index("pencil"), lax.axis_index("slab")
    barrier = pltpu.get_barrier_semaphore()
    for k in range(1, pencils):
        pl.semaphore_signal(
            barrier, inc=1, device_id={"pencil": lax.rem(me + k, pencils)}, device_id_type=MESH
        )
    for k in range(1, slabs):
        pl.semaphore_signal(
            barrier, inc=1, device_id={"slab": lax.rem(slab + k, slabs)}, device_id_type=MESH
        )
    pl.semaphore_wait(barrier, pencils + slabs - 2)

    def exchange(source, target, send, recv):
        copies = []
        for k in range(1, pencils):
            peer = lax.rem(me + k, pencils)
            copy = pltpu.make_async_remote_copy(
                src_ref=source.at[peer],
                dst_ref=target.at[me],
                send_sem=send.at[k - 1],
                recv_sem=recv.at[k - 1],
                device_id={"pencil": peer},
                device_id_type=MESH,
            )
            copy.start()
            copies.append(copy)
        target[me] = source[me]
        return copies

    def some(begin, end):
        def body(index, unused):
            base = index * group
            rhs = jnp.concatenate([u_ref[base + g] for g in range(group)], axis=1)
            answers = solve_group(rhs, coupling[0], width_ref, mixed_ref, depth_ref[...])
            for g in range(group):
                z_ref[base + g] = answers[g]
            return unused

        lax.fori_loop(begin, end, body, 0)

    groups = planes // group
    copies = exchange(faces_ref, held, send_one, recv_one)
    some(0, groups // 2)
    for copy in copies:
        copy.wait()
    value = jnp.zeros(held.shape[2:], F32)
    for d in range(pencils):
        solved[d, 0] = value
        if d < pencils - 1:
            value = held[d, 0] + chain[0, d] * value
    value = jnp.zeros(held.shape[2:], F32)
    for d in reversed(range(pencils)):
        solved[d, 1] = value
        if d > 0:
            value = held[d, 1] + chain[1, d] * solved[d, 0] + chain[2, d] * value
    copies = exchange(solved, final, send_two, recv_two)
    some(groups // 2, groups)
    for copy in copies:
        copy.wait()
    rhs = jnp.concatenate([final[:, side].reshape(width, depth) for side in range(2)], axis=1)
    answers = solve_group(rhs, coupling[0], width_ref, mixed_ref, depth_ref[...])
    for side in range(2):
        face_z[side] = answers[side]

    def correct(j, unused):
        z = z_ref[j] + into[0, j] * face_z[0] + into[1, j] * face_z[1]
        z_ref[j] = z
        ends[j] = ends_of(z)
        return unused

    lax.fori_loop(0, planes, correct, 0)
    copies = []
    for k in range(1, slabs):
        copy = pltpu.make_async_remote_copy(
            src_ref=ends,
            dst_ref=gathered.at[slab],
            send_sem=send_three.at[k - 1],
            recv_sem=recv_three.at[k - 1],
            device_id={"slab": lax.rem(slab + k, slabs)},
            device_id_type=MESH,
        )
        copy.start()
        copies.append(copy)
    gathered[slab] = ends[...]
    for copy in copies:
        copy.wait()
    zero = jnp.zeros((planes, width), F32)
    forward = [zero]
    for d in range(slabs - 1):
        forward.append(gathered[d, :, 1] + links[0, d] * forward[d])
    backward = [zero] * slabs
    for d in range(slabs - 1, 0, -1):
        backward[d - 1] = (
            gathered[d, :, 0] + links[1, d] * forward[d] + links[2, d] * backward[d]
        )
    carry_in, carry_next = forward[0], backward[0]
    for d in range(1, slabs):
        carry_in = jnp.where(slab == d, forward[d], carry_in)
        carry_next = jnp.where(slab == d, backward[d], carry_next)
    carry_ref[:, 0] = carry_in
    carry_ref[:, 1] = carry_next


def finish_kernel(group, rho_ref, z_ref, carry_ref, edge_ref, out_ref):
    width, depth = rho_ref.shape[1:]
    in_high, in_low = split(edge_ref[0:1])
    next_high, next_low = split(edge_ref[1:2])
    rhs = rows_of((in_high, in_high, in_low, next_high, next_high, next_low), depth)
    for g in range(group):
        a_high, a_low = split(carry_ref[g, 0:1])
        b_high, b_low = split(carry_ref[g, 1:2])
        lhs = rows_of((a_high, a_low, a_high, b_high, b_low, b_high), width)
        out_ref[g] = rho_ref[g] + z_ref[g] + dot(lhs, rhs, ((0,), (0,)))


def height_tables(strength, planes, count):
    root = (1.0 + 2.0 * strength + jnp.sqrt(1.0 + 4.0 * strength)) * 0.5
    ratio = strength / root
    log_ratio = jnp.log(ratio)

    def tail(index):
        return 1.0 - jnp.exp((2.0 * (index + 1.0)) * log_ratio)

    def power(index):
        return jnp.exp(index * log_ratio)

    base = (jnp.arange(count, dtype=F32) * planes)[:, None]
    j = jnp.arange(planes, dtype=F32)[None, :]
    pivots = tail(base + j) / (root * tail(base + j + 1.0))
    leave = power(planes - j) * tail(base + j) / tail(base + planes)
    base3, j3, m3 = base[:, :, None], j[:, :, None], j[:, None, :]
    distance = jnp.maximum(m3 - j3, 0.0)
    terms = (
        power(distance + m3 + 1.0)
        * (tail(base3 + j3) / tail(base3 + m3))
        * (tail(base3) / tail(base3 + m3 + 1.0))
    )
    enter = jnp.sum(jnp.where(m3 >= j3, terms, 0.0), axis=2)
    through = power(float(planes)) * tail(base[:, 0]) / tail(base[:, 0] + planes)
    return pivots, enter, leave, through


def per_device(density, source, coupling, width_inverse, height_inverse, depth_inverse):
    planes, width, depth = density.shape
    pencils, slabs = lax.axis_size("pencil"), lax.axis_size("slab")
    pencil, slab = lax.axis_index("pencil"), lax.axis_index("slab")
    size = depth_inverse.shape[1]
    group = 2
    smem = pl.BlockSpec(memory_space=pltpu.SMEM)
    params = pltpu.CompilerParams(
        dimension_semantics=("arbitrary",), vmem_limit_bytes=56 * 1024 * 1024
    )

    def whole(shape):
        return pl.BlockSpec(shape, lambda j: (0,) * len(shape))

    def per_plane(shape):
        return pl.BlockSpec(shape, lambda j: (j,) + (0,) * (len(shape) - 1))

    def plane_pairs(shape):
        return pl.BlockSpec(shape, lambda j: (0, j, 0, 0))

    vmem = pl.BlockSpec(memory_space=pltpu.VMEM)
    dma = pltpu.SemaphoreType.DMA
    strip = (2, planes, 1, width)
    halo = pl.pallas_call(
        lambda *refs: ends_kernel(slabs, 4, *refs),
        grid=(planes // 4,),
        out_shape=jax.ShapeDtypeStruct(strip, F32),
        in_specs=[per_plane((4, width, depth))],
        out_specs=whole(strip),
        scratch_shapes=[pltpu.VMEM(strip, F32), pltpu.VMEM(strip, F32), dma((2,)), dma((2,))],
        compiler_params=pltpu.CompilerParams(
            dimension_semantics=("arbitrary",),
            vmem_limit_bytes=56 * 1024 * 1024,
            collective_id=0,
            has_side_effects=True,
        ),
    )(density)

    pivots, enter, leave, through = height_tables(coupling[1], planes, pencils)
    own_pivots = lax.dynamic_index_in_dim(pivots, pencil, 0, False)
    into = jnp.stack(
        [
            lax.dynamic_index_in_dim(enter, pencil, 0, False),
            lax.dynamic_index_in_dim(leave, pencil, 0, False),
        ]
    )
    share = width // pencils
    partial, faces = pl.pallas_call(
        lambda *refs: height_kernel(planes, group, *refs),
        grid=(planes // group,),
        out_shape=(
            jax.ShapeDtypeStruct((planes, width, depth), F32),
            jax.ShapeDtypeStruct((pencils, 2, share, depth), F32),
        ),
        in_specs=[
            smem,
            smem,
            per_plane((group, width, depth)),
            per_plane((group, width, depth)),
            plane_pairs((2, group, 1, width)),
        ],
        out_specs=(whole((planes, width, depth)), whole((pencils, 2, share, depth))),
        scratch_shapes=[pltpu.VMEM((planes, width, depth), F32)],
        compiler_params=params,
    )(coupling, own_pivots, density, source, halo)

    w_high, w_low = split_outside(width_inverse)
    mixed = jnp.concatenate(
        [
            jnp.concatenate([w_high, w_high], axis=2),
            jnp.concatenate([w_low, jnp.zeros_like(w_low)], axis=2),
        ],
        axis=1,
    )
    matrix = lax.dynamic_index_in_dim(depth_inverse, slab, 0, False).T
    d_high, d_low = split_outside(matrix)
    depth_mixed = jnp.concatenate(
        [
            jnp.concatenate([d_high, d_low], axis=1),
            jnp.concatenate([d_high, jnp.zeros_like(d_low)], axis=1),
        ],
        axis=0,
    )
    strength = coupling[2]
    chain = jnp.stack([through, enter[:, 0], leave[:, 0]])
    links = strength * jnp.stack(
        [depth_inverse[:, size - 1, 0], depth_inverse[:, 0, 0], depth_inverse[:, 0, size - 1]]
    )
    pieces = pltpu.VMEM((pencils, 2, share, depth), F32)
    local, carries = pl.pallas_call(
        lambda *refs: lines_kernel(group, pencils, slabs, *refs),
        out_shape=(
            jax.ShapeDtypeStruct((planes, width, depth), F32),
            jax.ShapeDtypeStruct((planes, 2, width), F32),
        ),
        in_specs=[smem] * 4 + [vmem] * 5,
        out_specs=(vmem, vmem),
        scratch_shapes=[
            pieces,
            pieces,
            pieces,
            pltpu.VMEM((2, width, depth), F32),
            pltpu.VMEM((planes, 2, width), F32),
            pltpu.VMEM((slabs, planes, 2, width), F32),
            dma((pencils - 1,)),
            dma((pencils - 1,)),
            dma((pencils - 1,)),
            dma((pencils - 1,)),
            dma((slabs - 1,)),
            dma((slabs - 1,)),
        ],
        compiler_params=pltpu.CompilerParams(
            vmem_limit_bytes=56 * 1024 * 1024, collective_id=1, has_side_effects=True
        ),
    )(coupling, into, chain, links, partial, faces, width_inverse, mixed, depth_mixed)

    edges = strength * jnp.stack([matrix[0], matrix[size - 1]])
    return pl.pallas_call(
        lambda *refs: finish_kernel(group, *refs),
        grid=(planes // group,),
        out_shape=jax.ShapeDtypeStruct((planes, width, depth), F32),
        in_specs=[
            per_plane((group, width, depth)),
            per_plane((group, width, depth)),
            per_plane((group, 2, width)),
            whole((2, depth)),
        ],
        out_specs=per_plane((group, width, depth)),
        compiler_params=params,
    )(density, local, carries, edges)


def solution(mesh):
    in_specs = (P("pencil", None, "slab"), P("pencil", None, "slab"), P(), P(), P(), P())
    out_specs = P("pencil", None, "slab")
    return jax.shard_map(
        per_device, mesh=mesh, in_specs=in_specs, out_specs=out_specs, check_vma=False
    )
```

```python
import jax
import jax.numpy as jnp
from jax import lax
from jax.experimental import pallas as pl
from jax.experimental.pallas import tpu as pltpu
from jax.sharding import PartitionSpec as P

F32, BF16 = jnp.float32, jnp.bfloat16
MESH = pl.DeviceIdType.MESH


def split(value):
    high = value.astype(BF16)
    return high, (value - high.astype(F32)).astype(BF16)


def both(value, axis):
    return jnp.concatenate(split(value), axis=axis)


def dot(a, b, dims):
    return lax.dot_general(a, b, (dims, ((), ())), preferred_element_type=F32)


def ends_of(plane):
    width, depth = plane.shape
    row = lax.broadcasted_iota(jnp.int32, (depth, depth), 0)
    lane = lax.broadcasted_iota(jnp.int32, (depth, depth), 1)
    lines = []
    for column in (0, depth - 1):
        pieces = []
        for start in range(0, width, depth):
            edge = plane[start : start + depth, column : column + 1]
            pieces.append(jnp.sum(jnp.where(row == lane, edge, 0.0), axis=0, keepdims=True))
        lines.append(jnp.concatenate(pieces, axis=1))
    return jnp.concatenate(lines, axis=0)


def rows_of(pieces, width):
    row = lax.broadcasted_iota(jnp.int32, (16, width), 0)
    value = jnp.zeros((16, width), F32)
    for number, piece in enumerate(pieces):
        value = jnp.where(row == number, piece.astype(F32), value)
    return value.astype(BF16)


class Heights:
    def __init__(self, strength, planes, lanes):
        self.shape, self.planes = (1, lanes), planes
        strength = jnp.full(self.shape, strength, F32)
        self.root = (1.0 + 2.0 * strength + jnp.sqrt(1.0 + 4.0 * strength)) * 0.5
        self.log_ratio = jnp.log(strength / self.root)

    def power(self, index):
        return jnp.exp(jnp.full(self.shape, index, jnp.int32).astype(F32) * self.log_ratio)

    def tail(self, index):
        return 1.0 - self.power(2 * (index + 1))

    def pivot(self, index):
        return self.tail(index) / (self.root * self.tail(index + 1))

    def enter(self, device, j):
        base = device * self.planes
        return (
            self.power(j + 1)
            * (self.tail(base) / self.tail(base + self.planes))
            * (self.tail(self.planes - j - 1) / self.tail(0))
        )

    def leave(self, device, j):
        base = device * self.planes
        return self.power(self.planes - j) * (self.tail(base + j) / self.tail(base + self.planes))

    def through(self, device):
        return self.enter(device, self.planes - 1)


def ends_kernel(slabs, group, rho_ref, halo_ref, ends_ref, got_ref, send_sem, recv_sem):
    j = pl.program_id(0)
    me = lax.axis_index("slab")
    nxt, prv = lax.rem(me + 1, slabs), lax.rem(me + slabs - 1, slabs)
    barrier = pltpu.get_barrier_semaphore()

    @pl.when(j == 0)
    def _():
        for peer in (nxt, prv):
            pl.semaphore_signal(barrier, inc=1, device_id={"slab": peer}, device_id_type=MESH)

    for g in range(group):
        pair = ends_of(rho_ref[g])
        ends_ref[0, j * group + g] = pair[0:1]
        ends_ref[1, j * group + g] = pair[1:2]

    @pl.when(j == pl.num_programs(0) - 1)
    def _():
        pl.semaphore_wait(barrier, 2)
        copies = [
            pltpu.make_async_remote_copy(
                src_ref=ends_ref.at[1 - way],
                dst_ref=got_ref.at[way],
                send_sem=send_sem.at[way],
                recv_sem=recv_sem.at[way],
                device_id={"slab": peer},
                device_id_type=MESH,
            )
            for way, peer in ((0, nxt), (1, prv))
        ]
        for copy in copies:
            copy.start()
        for copy in copies:
            copy.wait()
        halo_ref[0] = jnp.where(me == 0, 0.0, got_ref[0])
        halo_ref[1] = jnp.where(me == slabs - 1, 0.0, got_ref[1])


def height_kernel(
    planes, group, coupling, rho_ref, source_ref, halo_ref, x_ref, faces_ref, kept_ref
):
    step = pl.program_id(0)
    width, depth = rho_ref.shape[1:]
    strength = coupling[1]
    row = lax.broadcasted_iota(jnp.int32, (width, depth), 0)
    lane = lax.broadcasted_iota(jnp.int32, (width, depth), 1)
    first = (lax.broadcasted_iota(jnp.int32, (1, depth), 1) == 0).astype(F32)
    last = (lax.broadcasted_iota(jnp.int32, (1, depth), 1) == depth - 1).astype(F32)
    units = rows_of((first, first, last, last), depth)
    heights = Heights(strength, planes, depth)
    base = lax.axis_index("pencil") * planes

    @pl.when(step == 0)
    def _():
        x_ref[planes - 1] = jnp.zeros((width, depth), F32)

    for g in range(group):
        j = step * group + g
        rho = rho_ref[g]
        below = jnp.where(row == 0, 0.0, pltpu.roll(rho, 1, 0))
        above = jnp.where(row == width - 1, 0.0, pltpu.roll(rho, width - 1, 0))
        before = jnp.where(lane == 0, 0.0, pltpu.roll(rho, 1, 1))
        after = jnp.where(lane == depth - 1, 0.0, pltpu.roll(rho, depth - 1, 1))
        left_high, left_low = split(halo_ref[0, g])
        right_high, right_low = split(halo_ref[1, g])
        edge = dot(rows_of((left_high, left_low, right_high, right_low), width), units, ((0,), (0,)))
        rhs = (
            2.0
            * (
                coupling[0] * (below + above - 2.0 * rho)
                + coupling[2] * (before + after + edge - 2.0 * rho)
            )
            + source_ref[g]
            + 2.0 * rho
        )
        kept_ref[j] = 2.0 * rho
        x_ref[j] = (rhs + strength * x_ref[lax.rem(j + planes - 1, planes)]) * heights.pivot(base + j)

    @pl.when(step == planes // group - 1)
    def _():
        shape = faces_ref.shape
        faces_ref[:, 0] = x_ref[planes - 1].reshape(shape[0], shape[2], shape[3])

        def back(count, unused):
            i = planes - 2 - count
            later = x_ref[i + 1]
            x_ref[i] = x_ref[i] + (strength * heights.pivot(base + i)) * later
            x_ref[i + 1] = later - kept_ref[i + 1]
            return unused

        lax.fori_loop(0, planes - 1, back, 0)
        faces_ref[:, 1] = x_ref[0].reshape(shape[0], shape[2], shape[3])
        x_ref[0] = x_ref[0] - kept_ref[0]


def solve_group(rhs, strength, width_ref, mixed_ref, depth_mixed):
    count, size = width_ref.shape[:2]
    depth = size
    total = rhs.shape[1]
    high, low = split(rhs)
    local, starts, stops = [], [], []
    for i in range(count):
        part = slice(i * size, (i + 1) * size)
        product = dot(mixed_ref[i], jnp.concatenate([high[part], low[part]], 0), ((1,), (0,)))
        local.append(product[:size] + product[size:])
        starts.append(strength * width_ref[i, :, 0:1])
        stops.append(strength * width_ref[i, :, size - 1 : size])
    carry = jnp.zeros((1, total), F32)
    ahead, heads = [], []
    for i in range(count):
        ahead.append(carry)
        heads.append(local[i][0:1] + starts[i][0:1] * carry)
        carry = local[i][size - 1 :] + starts[i][size - 1 :] * carry
    carry = jnp.zeros((1, total), F32)
    solved = [None] * count
    for i in reversed(range(count)):
        solved[i] = local[i] + starts[i] * ahead[i] + stops[i] * carry
        carry = heads[i] + stops[i][0:1] * carry
    solved = jnp.concatenate(solved, axis=0)
    answers = []
    for start in range(0, total, depth):
        product = dot(both(solved[:, start : start + depth], 1), depth_mixed, ((1,), (0,)))
        answers.append(product[:, :depth] + product[:, depth:])
    return answers


def lines_kernel(
    group, pencils, slabs,
    coupling,
    u_hbm, faces_ref, width_ref, depth_ref,
    z_hbm, carry_ref,
    u_ref, z_ref, mixed_ref, mixed_depth,
    held, solved, final, face_z, ends, gathered,
    send_one, recv_one, send_two, recv_two, send_three, recv_three, load_sem, store_sem,
):
    planes, width, depth = u_ref.shape
    groups = planes // group
    count, size = width_ref.shape[:2]
    me, slab = lax.axis_index("pencil"), lax.axis_index("slab")
    barrier = pltpu.get_barrier_semaphore()
    for k in range(1, pencils):
        pl.semaphore_signal(
            barrier, inc=1, device_id={"pencil": lax.rem(me + k, pencils)}, device_id_type=MESH
        )
    for k in range(1, slabs):
        pl.semaphore_signal(
            barrier, inc=1, device_id={"slab": lax.rem(slab + k, slabs)}, device_id_type=MESH
        )

    def load(index):
        part = pl.ds(index * group, group)
        return pltpu.make_async_copy(u_hbm.at[part], u_ref.at[part], load_sem.at[index])

    def store(j):
        return pltpu.make_async_copy(z_ref.at[j], z_hbm.at[j], store_sem.at[j])

    for index in range(groups):
        load(index).start()
    for i in range(count):
        high, low = split(width_ref[i])
        mixed_ref[i, :size, :size] = high
        mixed_ref[i, :size, size:] = high
        mixed_ref[i, size:, :size] = low
        mixed_ref[i, size:, size:] = jnp.zeros_like(low)
    high, low = split(depth_ref[slab])
    mixed_depth[:size, :size] = high
    mixed_depth[size:, :size] = high
    mixed_depth[:size, size:] = low
    mixed_depth[size:, size:] = jnp.zeros_like(low)
    pl.semaphore_wait(barrier, pencils + slabs - 2)
    heights = Heights(coupling[1], planes, depth)

    def exchange(source, target, send, recv):
        copies = []
        for k in range(1, pencils):
            peer = lax.rem(me + k, pencils)
            copy = pltpu.make_async_remote_copy(
                src_ref=source.at[peer],
                dst_ref=target.at[me],
                send_sem=send.at[k - 1],
                recv_sem=recv.at[k - 1],
                device_id={"pencil": peer},
                device_id_type=MESH,
            )
            copy.start()
            copies.append(copy)
        target[me] = source[me]
        return copies

    def some(begin, end):
        def body(index, unused):
            base = index * group
            load(index).wait()
            rhs = jnp.concatenate([u_ref[base + g] for g in range(group)], axis=1)
            answers = solve_group(rhs, coupling[0], width_ref, mixed_ref, mixed_depth[...])
            for g in range(group):
                z_ref[base + g] = answers[g]
                ends[base + g] = ends_of(answers[g])
            return unused

        lax.fori_loop(begin, end, body, 0)

    copies = exchange(faces_ref, held, send_one, recv_one)
    some(0, groups // 2)
    for copy in copies:
        copy.wait()
    value = jnp.zeros(held.shape[2:], F32)
    for d in range(pencils):
        solved[d, 0] = value
        if d < pencils - 1:
            value = held[d, 0] + heights.through(d) * value
    value = jnp.zeros(held.shape[2:], F32)
    for d in reversed(range(pencils)):
        solved[d, 1] = value
        if d > 0:
            value = held[d, 1] + heights.enter(d, 0) * solved[d, 0] + heights.leave(d, 0) * value
    copies = exchange(solved, final, send_two, recv_two)
    some(groups // 2, groups)
    for copy in copies:
        copy.wait()
    rhs = jnp.concatenate([final[:, side].reshape(width, depth) for side in range(2)], axis=1)
    answers = solve_group(rhs, coupling[0], width_ref, mixed_ref, mixed_depth[...])
    for side in range(2):
        face_z[side] = answers[side]
    edge_enter, edge_leave = ends_of(answers[0]), ends_of(answers[1])

    def correct_ends(j, unused):
        enter, leave = heights.enter(me, j)[:, 0:1], heights.leave(me, j)[:, 0:1]
        ends[j] = ends[j] + enter * edge_enter + leave * edge_leave
        return unused

    def correct(j, unused):
        enter, leave = heights.enter(me, j), heights.leave(me, j)
        z_ref[j] = z_ref[j] + enter * face_z[0] + leave * face_z[1]
        store(j).start()
        return unused

    def finish_store(j, unused):
        store(j).wait()
        return unused

    lax.fori_loop(0, planes, correct_ends, 0)
    copies = []
    for k in range(1, slabs):
        copy = pltpu.make_async_remote_copy(
            src_ref=ends,
            dst_ref=gathered.at[slab],
            send_sem=send_three.at[k - 1],
            recv_sem=recv_three.at[k - 1],
            device_id={"slab": lax.rem(slab + k, slabs)},
            device_id_type=MESH,
        )
        copy.start()
        copies.append(copy)
    gathered[slab] = ends[...]
    lax.fori_loop(0, planes, correct, 0)
    for copy in copies:
        copy.wait()

    def link(d, row, column):
        return coupling[2] * depth_ref[d, row : row + 1, column : column + 1]

    zero = jnp.zeros((planes, width), F32)
    forward = [zero]
    for d in range(slabs - 1):
        forward.append(gathered[d, :, 1] + link(d, size - 1, 0) * forward[d])
    backward = [zero] * slabs
    for d in range(slabs - 1, 0, -1):
        backward[d - 1] = (
            gathered[d, :, 0] + link(d, 0, 0) * forward[d] + link(d, 0, size - 1) * backward[d]
        )
    carry_in, carry_next = forward[0], backward[0]
    for d in range(1, slabs):
        carry_in = jnp.where(slab == d, forward[d], carry_in)
        carry_next = jnp.where(slab == d, backward[d], carry_next)
    carry_ref[:, 0] = carry_in
    carry_ref[:, 1] = carry_next
    lax.fori_loop(0, planes, finish_store, 0)


def finish_kernel(group, coupling, rho_ref, z_ref, carry_ref, depth_ref, out_ref):
    width, depth = rho_ref.shape[1:]
    slab, size = lax.axis_index("slab"), depth_ref.shape[1]
    in_high, in_low = split(coupling[2] * depth_ref[slab, 0:1])
    next_high, next_low = split(coupling[2] * depth_ref[slab, size - 1 : size])
    rhs = rows_of((in_high, in_high, in_low, next_high, next_high, next_low), depth)
    for g in range(group):
        a_high, a_low = split(carry_ref[g, 0:1])
        b_high, b_low = split(carry_ref[g, 1:2])
        lhs = rows_of((a_high, a_low, a_high, b_high, b_low, b_high), width)
        out_ref[g] = rho_ref[g] + z_ref[g] + dot(lhs, rhs, ((0,), (0,)))


def per_device(density, source, coupling, width_inverse, height_inverse, depth_inverse):
    planes, width, depth = density.shape
    pencils, slabs = lax.axis_size("pencil"), lax.axis_size("slab")
    size = depth_inverse.shape[1]
    group = 2
    smem = pl.BlockSpec(memory_space=pltpu.SMEM)
    params = pltpu.CompilerParams(
        dimension_semantics=("arbitrary",), vmem_limit_bytes=56 * 1024 * 1024
    )

    def whole(shape):
        return pl.BlockSpec(shape, lambda j: (0,) * len(shape))

    def per_plane(shape):
        return pl.BlockSpec(shape, lambda j: (j,) + (0,) * (len(shape) - 1))

    def plane_pairs(shape):
        return pl.BlockSpec(shape, lambda j: (0, j, 0, 0))

    vmem = pl.BlockSpec(memory_space=pltpu.VMEM)
    hbm = pl.BlockSpec(memory_space=pl.ANY)
    blocks = width_inverse.shape[0]
    dma = pltpu.SemaphoreType.DMA
    strip = (2, planes, 1, width)
    halo = pl.pallas_call(
        lambda *refs: ends_kernel(slabs, 4, *refs),
        grid=(planes // 4,),
        out_shape=jax.ShapeDtypeStruct(strip, F32),
        in_specs=[per_plane((4, width, depth))],
        out_specs=whole(strip),
        scratch_shapes=[pltpu.VMEM(strip, F32), pltpu.VMEM(strip, F32), dma((2,)), dma((2,))],
        compiler_params=pltpu.CompilerParams(
            dimension_semantics=("arbitrary",),
            vmem_limit_bytes=56 * 1024 * 1024,
            collective_id=0,
            has_side_effects=True,
        ),
    )(density)

    share = width // pencils
    partial, faces = pl.pallas_call(
        lambda *refs: height_kernel(planes, group, *refs),
        grid=(planes // group,),
        out_shape=(
            jax.ShapeDtypeStruct((planes, width, depth), F32),
            jax.ShapeDtypeStruct((pencils, 2, share, depth), F32),
        ),
        in_specs=[
            smem,
            per_plane((group, width, depth)),
            per_plane((group, width, depth)),
            plane_pairs((2, group, 1, width)),
        ],
        out_specs=(whole((planes, width, depth)), whole((pencils, 2, share, depth))),
        scratch_shapes=[pltpu.VMEM((planes, width, depth), F32)],
        compiler_params=params,
    )(coupling, density, source, halo)

    pieces = pltpu.VMEM((pencils, 2, share, depth), F32)
    local, carries = pl.pallas_call(
        lambda *refs: lines_kernel(group, pencils, slabs, *refs),
        out_shape=(
            jax.ShapeDtypeStruct((planes, width, depth), F32),
            jax.ShapeDtypeStruct((planes, 2, width), F32),
        ),
        in_specs=[smem, hbm, vmem, vmem, vmem],
        out_specs=(hbm, vmem),
        scratch_shapes=[
            pltpu.VMEM((planes, width, depth), F32),
            pltpu.VMEM((planes, width, depth), F32),
            pltpu.VMEM((blocks, 2 * size, 2 * size), BF16),
            pltpu.VMEM((2 * size, 2 * size), BF16),
            pieces,
            pieces,
            pieces,
            pltpu.VMEM((2, width, depth), F32),
            pltpu.VMEM((planes, 2, width), F32),
            pltpu.VMEM((slabs, planes, 2, width), F32),
            dma((pencils - 1,)),
            dma((pencils - 1,)),
            dma((pencils - 1,)),
            dma((pencils - 1,)),
            dma((slabs - 1,)),
            dma((slabs - 1,)),
            dma((planes // group,)),
            dma((planes,)),
        ],
        compiler_params=pltpu.CompilerParams(
            vmem_limit_bytes=56 * 1024 * 1024, collective_id=1, has_side_effects=True
        ),
    )(coupling, partial, faces, width_inverse, depth_inverse)

    return pl.pallas_call(
        lambda *refs: finish_kernel(group, *refs),
        grid=(planes // group,),
        out_shape=jax.ShapeDtypeStruct((planes, width, depth), F32),
        in_specs=[
            smem,
            per_plane((group, width, depth)),
            per_plane((group, width, depth)),
            per_plane((group, 2, width)),
            whole(depth_inverse.shape),
        ],
        out_specs=per_plane((group, width, depth)),
        compiler_params=params,
    )(coupling, density, local, carries, depth_inverse)


def solution(mesh):
    in_specs = (P("pencil", None, "slab"), P("pencil", None, "slab"), P(), P(), P(), P())
    out_specs = P("pencil", None, "slab")
    return jax.shard_map(
        per_device, mesh=mesh, in_specs=in_specs, out_specs=out_specs, check_vma=False
    )
```
